512 devices in a mesh: gx: 16 (over y_lo, z), gy: 4 (over x), col: 8 (over y_hi, core).
Axes of the slice: x: 4, y: 8 (y_hi: 4, y_lo: 2; y = y_hi * 2 + y_lo), z: 8, core: 2. Of those that a mesh axis runs over, the one named last changes fastest.
Arguments:
- fields: bfloat16 [8, 128, 128, 32, 128], P('col', 'gx', 'gy'), may hold values from -6 to 6
- spectral: bfloat16 [1, 16, 16, 2, 32, 32, 16], P(None, 'gx', 'gy', None, None, 'col'), may hold values from -0.75 to 0.75
- skip_weight: bfloat16 [1, 32, 32], replicated, may hold values from -1 to 1
- skip_bias: float32 [1, 32], replicated, may hold values from -3 to 3
- norm_gain: float32 [1, 32], replicated, may hold values from 0.5 to 1.5
- norm_shift: float32 [1, 32], replicated, may hold values from -3 to 3
Outputs:
- activations: bfloat16 [8, 128, 128, 32, 128], P('col', 'gx', 'gy')
The draws below stay inside these ranges and needn't reach their ends.
All inputs are finite; a program needn't handle non-finite values.
Results may differ from the reference program's by a relative error of at most 0.012.
Values may be sent and summed in bfloat16 or wider, within the bound.
A program may use at most 64 MiB of HBM per device.

```python
import math
import jax
import jax.numpy as jnp
from jax import lax

X = 128
Y = 128
Z = 128
C = 32
MX = 16
MY = 16
MZ = 16
LAYERS = 1
SAMPLES = 8


def block_levels(own_key, shape, split, low, largest):
    def one(dim, shards_of):
        draws = jax.random.uniform(jax.random.fold_in(jax.random.fold_in(own_key, 6), dim), (shards_of,), jnp.float32, low / len(split), largest / len(split))
        return jnp.repeat(jnp.exp(draws), shape[dim] // shards_of).reshape((-1,) + (1,) * (len(shape) - dim - 1))

    level = one(*split[0])
    for cut in split[1:]:
        level = level * one(*cut)
    return level


def scatter_about(stream_key, dims, scale, bound, split=(), kind=jnp.bfloat16):
    gain = block_levels(stream_key, dims, split, -0.22, 0.18) if split else 1.0
    array = jax.random.normal(stream_key, dims, jnp.float32) * scale * gain
    return jnp.minimum(jnp.maximum(array, -bound), bound).astype(kind)


def setup_inputs(seed: int = 0) -> dict:
    keys = jax.random.split(jax.random.key(seed), 7)
    fields = scatter_about(keys[0], (SAMPLES, X, Y, C, Z), 1.0, 6.0, ((0, 8), (1, 16), (2, 4)))
    spectral = scatter_about(keys[1], (LAYERS, MX, MY, 2, C, C, MZ), (2 * C) ** -0.5, 0.75, ((1, 16), (2, 4), (5, 8)))
    skip_weight = scatter_about(keys[2], (LAYERS, C, C), C ** -0.5, 1.0)
    skip_bias = scatter_about(keys[3], (LAYERS, C), 0.5, 3.0, (), jnp.float32)
    norm_gain = jnp.clip(jax.random.uniform(keys[4], (LAYERS, C), jnp.float32, 0.5, 1.5), 0.5, 1.5)
    norm_shift = scatter_about(keys[5], (LAYERS, C), 0.5, 3.0, (), jnp.float32)
    return dict(fields=fields, spectral=spectral, skip_weight=skip_weight, skip_bias=skip_bias, norm_gain=norm_gain, norm_shift=norm_shift)


norm_eps = 1e-05

def signed_freqs(count):
    index = jnp.arange(count, dtype=jnp.int32)
    return jnp.where(index < count // 2, index, index - count)

def angles(positions, frequency, length):
    turn_count = positions[:, None] * frequency[None, :] % length
    return turn_count.astype(jnp.float32) * (2.0 * math.pi / length)

def forward_table(positions, frequency, length, factor):
    phase_angle = angles(positions, frequency, length)
    cosine = jnp.cos(phase_angle) * factor
    sine_part = jnp.sin(phase_angle) * factor
    from_real = jnp.stack([cosine, -sine_part], axis=-1)
    from_imag = jnp.stack([sine_part, cosine], axis=-1)
    return jnp.stack([from_real, from_imag], axis=1)

def inverse_table(frequency, positions, length):
    phase_angle = angles(positions, frequency, length).T
    cosine = jnp.cos(phase_angle)
    sine_part = jnp.sin(phase_angle)
    from_real = jnp.stack([cosine, sine_part], axis=-1)
    from_imag = jnp.stack([-sine_part, cosine], axis=-1)
    return jnp.stack([from_real, from_imag], axis=1)

def depth_tables(length, count):
    frequency = jnp.arange(count, dtype=jnp.int32)
    phase_angle = angles(jnp.arange(length, dtype=jnp.int32), frequency, length)
    forward = jnp.concatenate([jnp.cos(phase_angle), -jnp.sin(phase_angle)], axis=1)
    backward = jnp.concatenate([jnp.cos(phase_angle).T, -jnp.sin(phase_angle).T], axis=0)
    return (forward.astype(jnp.bfloat16), backward.astype(jnp.bfloat16))

def mix_modes(spectrum, weight):

    def contract(left, right):
        return jnp.einsum('abcz,abcdz->abdz', left, right, preferred_element_type=jnp.float32, precision=lax.Precision.HIGHEST)
    real_in = spectrum[:, :, :, 0]
    imag_in = spectrum[:, :, :, 1]
    real_weight = weight[:, :, 0]
    imag_weight = weight[:, :, 1]
    real_out = contract(real_in, real_weight) - contract(imag_in, imag_weight)
    imag_out = contract(real_in, imag_weight) + contract(imag_in, real_weight)
    return jnp.stack([real_out, imag_out], axis=3)

def finish(spectral_part, skip_part, offset, scaling, shift_term):
    pre_norm = spectral_part + skip_part + offset[:, None]
    centre = lax.optimization_barrier(jnp.mean(pre_norm, axis=2, keepdims=True))
    spread = lax.optimization_barrier(jnp.mean(jnp.square(pre_norm - centre), axis=2, keepdims=True))
    normed = (pre_norm - centre) * lax.rsqrt(spread + norm_eps) * scaling[:, None] + shift_term[:, None]
    return jax.nn.gelu(normed, approximate=False).astype(jnp.bfloat16)

def sample_layers(sample, spectral, skip_weight, skip_bias, norm_gain, norm_shift):
    highest = lax.Precision.HIGHEST
    depth_forward, depth_backward = depth_tables(Z, MZ)
    first_cells = jnp.arange(X, dtype=jnp.int32)
    second_cells = jnp.arange(Y, dtype=jnp.int32)
    second_forward = forward_table(second_cells, signed_freqs(MY), Y, 1.0).astype(jnp.bfloat16)
    first_forward = forward_table(first_cells, signed_freqs(MX), X, 1.0 / math.sqrt(X * Y * Z))
    first_inverse = inverse_table(signed_freqs(MX), first_cells, X).astype(jnp.bfloat16)
    second_inverse = inverse_table(signed_freqs(MY), second_cells, Y)
    inverse_scale = 1.0 / math.sqrt(MX * MY * MZ)
    hidden = sample
    for layer_index in range(LAYERS):
        amplitude = jnp.dot(hidden.reshape(-1, Z).astype(jnp.float32), depth_forward.astype(jnp.float32), precision=highest)
        amplitude = amplitude.astype(jnp.bfloat16).reshape(X, Y, C, 2, MZ)
        along_second = jnp.einsum('xycrz,yrks->xkcsz', amplitude.astype(jnp.float32), second_forward.astype(jnp.float32), precision=highest)
        spectrum_sum = jnp.einsum('xkcsz,xsjt->jkctz', along_second, first_forward, precision=highest)
        spectrum = spectrum_sum.astype(jnp.bfloat16)
        mixed_modes = mix_modes(spectrum.astype(jnp.float32), spectral[layer_index].astype(jnp.float32)).astype(jnp.bfloat16)
        rows_first = jnp.einsum('jkcsz,jsxt->xkctz', mixed_modes.astype(jnp.float32), first_inverse.astype(jnp.float32), precision=highest)
        rows_both = jnp.einsum('xkcsz,ksyt->xyctz', rows_first, second_inverse, precision=highest).astype(jnp.bfloat16)
        spectral_part = jnp.dot(rows_both.reshape(-1, 2 * MZ).astype(jnp.float32), depth_backward.astype(jnp.float32), precision=highest)
        spectral_part = spectral_part.reshape(X, Y, C, Z) * inverse_scale
        skip_part = jnp.einsum('oc,xycz->xyoz', skip_weight[layer_index].astype(jnp.float32), hidden.astype(jnp.float32), precision=highest)
        hidden = finish(spectral_part, skip_part, skip_bias[layer_index], norm_gain[layer_index], norm_shift[layer_index])
    return hidden

def reference(fields, spectral, skip_weight, skip_bias, norm_gain, norm_shift):

    def per_sample(sample):
        return sample_layers(sample, spectral, skip_weight, skip_bias, norm_gain, norm_shift)
    return lax.map(per_sample, fields)
```

```python
import functools
import math

import jax
import jax.numpy as jnp
import numpy as np
from jax import lax
from jax.experimental import pallas as pl
from jax.experimental.pallas import tpu as pltpu
from jax.sharding import PartitionSpec as P

MESH = pl.DeviceIdType.MESH
F32, BF16 = jnp.float32, jnp.bfloat16

N = 128
M = 16
C = 32
GX, GY, COL = 16, 4, 8
TX, TY = N // GX, N // GY
KY = M // GY
LANES = 2 * KY * M
PEER = GY * LANES
HALF = C // 2
NORM_EPS = 1e-05

FAR_X = [(dy, dz) for dz in (4, 3, 5, 2, 6, 1, 7, 0) for dy in (1, 0) if (dy, dz) != (0, 0)]
FAR_Y = (2, 1, 3)
FAR_COL = (2, 1, 3)


def signed(k):
    return np.where(k < M // 2, k, k - M)


def base_tables():
    turn = np.outer(np.arange(N), np.arange(M)) % N * (2.0 * math.pi / N)
    cosine, sine = np.tile(np.cos(turn), (1, KY)), np.tile(np.sin(turn), (1, KY))
    first = np.concatenate([cosine, -sine], axis=1)
    second = np.concatenate([-sine, -cosine], axis=1)
    return np.stack([first, second]).astype(np.float32)


def turn_tables():
    out = np.zeros((GY, 2, TY, GY, LANES), np.float32)
    for g in range(GY):
        for step in range(GY):
            ky = (g + step) % GY * KY + np.arange(KY)
            turn = np.outer(g * TY + np.arange(TY), signed(ky)) % N * (2.0 * math.pi / N)
            out[g, 0, :, step] = np.tile(np.repeat(np.cos(turn), M, axis=1), (1, 2))
            out[g, 1, :, step] = np.tile(np.repeat(np.sin(turn), M, axis=1), (1, 2))
    return out.reshape(GY, 2 * TY * GY, LANES)


def first_tables():
    f = np.arange(M // 2 + 1)
    out = np.zeros((GX, 2, f.size, TX), np.float32)
    for g in range(GX):
        turn = np.outer(f, g * TX + np.arange(TX)) % N * (2.0 * math.pi / N)
        out[g, 0], out[g, 1] = np.cos(turn), np.sin(turn)
    out = out.reshape(GX, -1, 1)
    return np.ascontiguousarray(np.broadcast_to(out, (GX, out.shape[1], LANES)))


def turned(v):
    lane = lax.broadcasted_iota(jnp.int32, v.shape, v.ndim - 1)
    swapped = pltpu.roll(v, LANES // 2, v.ndim - 1)
    return jnp.where(lane < LANES // 2, swapped, -swapped)


def modes_kernel(
    h_hbm, w_hbm, skw_hbm, par_hbm, base_hbm, turn_hbm, first_hbm,
    rows_ref, table_ref, skip_ref, affine_ref,
    hbuf, wraw, skw, par, base, turn, first,
    zsend, arecv, pm, brecv, spec, mixf, wbuf, mrecv,
    hsem, lsem, asend, arcv, bsend, brcv, csend, crcv, dsend, drcv, wsend, wrcv, vsend, vrcv,
):
    gx, gy, col = lax.axis_index("gx"), lax.axis_index("gy"), lax.axis_index("col")
    y_lo, z = gx // 8, gx % 8
    y_hi, core = col // 2, col % 2
    sibling = col + 1 - 2 * core

    def x_peer(dy, dz):
        return (y_lo + dy) % 2 * 8 + (z + dz) % 8

    def x_from(dy, dz):
        return (y_lo + dy) % 2 * 8 + (z + 8 - dz) % 8

    loads = [
        pltpu.make_async_copy(base_hbm, base, lsem.at[0]),
        pltpu.make_async_copy(turn_hbm.at[gy], turn, lsem.at[1]),
        pltpu.make_async_copy(w_hbm, wraw, lsem.at[2]),
        pltpu.make_async_copy(skw_hbm, skw, lsem.at[3]),
        pltpu.make_async_copy(par_hbm, par, lsem.at[4]),
        pltpu.make_async_copy(first_hbm.at[gx], first, lsem.at[5]),
    ]
    for cp in loads[:2]:
        cp.start()
    hload = [
        pltpu.make_async_copy(
            h_hbm.at[:, pl.ds(8 * q, 8)], hbuf.at[:, pl.ds(8 * q, 8)], hsem.at[q]
        )
        for q in range(4)
    ]
    for cp in hload:
        cp.start()
    for cp in loads[2:]:
        cp.start()

    barrier = pltpu.get_barrier_semaphore()
    for dy, dz in FAR_X:
        pl.semaphore_signal(barrier, 1, device_id={"gx": x_peer(dy, dz)}, device_id_type=MESH)
    for k in FAR_Y:
        pl.semaphore_signal(barrier, 1, device_id={"gy": (gy + k) % GY}, device_id_type=MESH)
    for k in FAR_COL:
        pl.semaphore_signal(
            barrier, 1, device_id={"col": (y_hi + k) % 4 * 2 + core}, device_id_type=MESH
        )
    pl.semaphore_signal(barrier, 1, device_id={"col": sibling}, device_id_type=MESH)

    for cp in loads[:2]:
        cp.wait()

    def table_row(y, carry):
        for k in range(GY):
            cosine = turn[pl.ds(y * GY + k, 1), :]
            sine = turn[pl.ds(TY * GY + y * GY + k, 1), :]
            table_ref[pl.ds(pl.multiple_of(y * N, N), N), k * LANES : (k + 1) * LANES] = (
                base[0] * cosine + base[1] * sine
            ).astype(BF16)
        return carry

    lax.fori_loop(0, TY, table_row, 0)
    for cp in hload:
        cp.wait()
    cells = jnp.concatenate([hbuf[:, y].reshape(TX * C, N) for y in range(TY)], axis=1)
    local = jnp.dot(cells, table_ref[...], preferred_element_type=F32)
    for k in range(GY):
        part = local[:, k * LANES : (k + 1) * LANES].astype(BF16).reshape(TX, 2, HALF, LANES)
        for half in range(2):
            zsend[k, half] = part[:, half]

    pl.semaphore_wait(barrier, len(FAR_X) + len(FAR_Y) + len(FAR_COL) + 1)

    a_copies = {}
    for half in range(2):
        for k in FAR_Y:
            a_copies[k, half] = pltpu.make_async_remote_copy(
                zsend.at[k, half], arecv.at[k - 1, half],
                asend.at[k - 1, half], arcv.at[k - 1, half],
                device_id={"gy": (gy + k) % GY}, device_id_type=MESH,
            )
            a_copies[k, half].start()

    loads[2].wait()
    for d in range(C // COL):
        block = jnp.concatenate(
            [wraw[k, s, d].astype(F32) for s in range(2) for k in range(KY)], axis=0
        )
        wbuf[col, d] = block.T.astype(BF16)
    w_copies = [
        pltpu.make_async_remote_copy(
            wbuf.at[col], wbuf.at[col], wsend.at[i], wrcv.at[i],
            device_id={"col": (y_hi + k) % 4 * 2 + core}, device_id_type=MESH,
        )
        for i, k in enumerate(FAR_COL)
    ]
    for cp in w_copies:
        cp.start()
    v_copies = [
        pltpu.make_async_remote_copy(
            wbuf.at[col], wbuf.at[col], vsend.at[3], vrcv.at[3],
            device_id={"col": sibling}, device_id_type=MESH,
        )
    ]
    v_copies[0].start()

    for cp in loads[3:]:
        cp.wait()
    wide = [jnp.broadcast_to(par[i : i + 1, :], (N, C)).T for i in range(3)]
    affine_ref[0] = wide[1]
    affine_ref[1] = wide[2]
    bias = wide[0] - jnp.mean(wide[0], axis=0, keepdims=True)
    pick = (
        lax.broadcasted_iota(jnp.int32, (C, TX * C), 1) % C
        == lax.broadcasted_iota(jnp.int32, (C, TX * C), 0)
    )
    spread = jnp.dot(skw[...], pick.astype(F32).astype(BF16), preferred_element_type=F32)
    spread = jnp.broadcast_to(spread[None], (TX, C, TX * C)).reshape(TX * C, TX * C)
    same = (
        lax.broadcasted_iota(jnp.int32, (TX * C, TX * C), 0) // C
        == lax.broadcasted_iota(jnp.int32, (TX * C, TX * C), 1) // C
    )
    diagonal = jnp.where(same, spread, 0.0).astype(BF16)

    def skip_pair(i, carry):
        pair = [hbuf[:, 2 * i + j].reshape(TX * C, N) for j in range(2)]
        out = jnp.dot(diagonal, jnp.concatenate(pair, axis=1), preferred_element_type=F32)
        for j in range(2):
            value = out[:, j * N : (j + 1) * N].reshape(TX, C, N)
            value = value - jnp.mean(value, axis=1, keepdims=True) + bias[None]
            skip_ref[2 * i + j] = value
        return carry

    lax.fori_loop(0, TY // 2, skip_pair, 0)

    b_copies = {}
    for half in range(2):
        for k in FAR_Y:
            a_copies[k, half].wait_recv()
        here, there = [], []
        for x in range(TX):
            v = zsend[0, half, x].astype(F32)
            for k in range(3):
                v = v + arecv[k, half, x].astype(F32)
            here.append(v)
            there.append(turned(v))
        for f in range(M // 2 + 1):
            even = odd = None
            for x in range(TX):
                if f == 0:
                    even = here[x] if even is None else even + here[x]
                    continue
                r = f * TX + x
                a = here[x] * first[r : r + 1, :]
                b = there[x] * first[9 * TX + r : 9 * TX + r + 1, :]
                even = a if even is None else even + a
                odd = b if odd is None else odd + b
            if f == 0:
                pm[half, 0] = even.astype(BF16)
                continue
            if f < M // 2:
                pm[half, f] = (even + odd).astype(BF16)
            pm[half, M - f] = (even - odd).astype(BF16)
        for i, (dy, dz) in enumerate(FAR_X):
            to = x_peer(dy, dz)
            b_copies[i, half] = pltpu.make_async_remote_copy(
                pm.at[half, to], brecv.at[i, half], bsend.at[i, half], brcv.at[i, half],
                device_id={"gx": to}, device_id_type=MESH,
            )
            b_copies[i, half].start()

    for i, k in enumerate(FAR_COL):
        w_copies[i].wait_recv()
        slot = (y_hi + 4 - k) % 4 * 2 + core
        v_copies.append(
            pltpu.make_async_remote_copy(
                wbuf.at[slot], wbuf.at[slot], vsend.at[i], vrcv.at[i],
                device_id={"col": sibling}, device_id_type=MESH,
            )
        )
        v_copies[-1].start()

    scale = 1.0 / math.sqrt(N * N * N)
    for half in range(2):
        total = pm[half, gx].astype(F32)
        for i in range(len(FAR_X)):
            b_copies[i, half].wait_recv()
        for i in range(len(FAR_X)):
            total = total + brecv[i, half].astype(F32)
        spec[half * HALF : (half + 1) * HALF, :] = (total * scale).astype(BF16).astype(F32)
    for cp in v_copies:
        cp.wait_recv()

    straight = spec[...]
    crossed = pltpu.roll(straight, LANES // 2, 1)
    lane = lax.broadcasted_iota(jnp.int32, (8, LANES), 1)
    for g in range(4):
        weight = wbuf[2 * g : 2 * g + 2].astype(F32).reshape(8, C, LANES)
        a = jnp.sum(weight * straight[None], axis=1)
        b = jnp.sum(weight * crossed[None], axis=1)
        mixed = jnp.where(
            lane < LANES // 2, a - pltpu.roll(a, LANES // 2, 1), b + pltpu.roll(b, LANES // 2, 1)
        )
        mixf[8 * g : 8 * g + 8, :] = mixed
    mixed = mixf[...]
    mixed = (mixed - jnp.mean(mixed, axis=0, keepdims=True)) * (1.0 / math.sqrt(M * M * M))
    mixed = mixed.astype(BF16)

    c_copies = {}
    for half in range(2):
        mrecv[gx, half] = mixed[half * HALF : (half + 1) * HALF]
        for i, (dy, dz) in enumerate(FAR_X):
            c_copies[i, half] = pltpu.make_async_remote_copy(
                mrecv.at[gx, half], mrecv.at[gx, half], csend.at[i, half], crcv.at[i, half],
                device_id={"gx": x_peer(dy, dz)}, device_id_type=MESH,
            )
            c_copies[i, half].start()

    d_copies = {}
    for half in range(2):
        for i in range(len(FAR_X)):
            c_copies[i, half].wait_recv()
        zero = mrecv[0, half].astype(F32)
        out = [zero for _ in range(TX)]
        for f in range(1, M // 2 + 1):
            low = mrecv[M - f, half].astype(F32)
            if f < M // 2:
                high = mrecv[f, half].astype(F32)
                even, odd = high + low, turned(low - high)
            else:
                even, odd = low, turned(low)
            for x in range(TX):
                r = f * TX + x
                out[x] = out[x] + even * first[r : r + 1, :]
                out[x] = out[x] + odd * first[9 * TX + r : 9 * TX + r + 1, :]
        part = pl.ds(half * HALF, HALF)
        for x in range(TX):
            rows_ref[0, x, part, :] = out[x].astype(BF16)
        for k in FAR_Y:
            d_copies[k, half] = pltpu.make_async_remote_copy(
                rows_ref.at[0, :, part, :], rows_ref.at[k, :, part, :],
                dsend.at[k - 1, half], drcv.at[k - 1, half],
                device_id={"gy": (gy + GY - k) % GY}, device_id_type=MESH,
            )
            d_copies[k, half].start()

    for cp in d_copies.values():
        cp.wait_recv()
    for cp in [*a_copies.values(), *w_copies, *b_copies.values(), *v_copies,
               *c_copies.values(), *d_copies.values()]:
        cp.wait_send()


def finish_kernel(rows_ref, table_ref, skip_ref, affine_ref, out_hbm, obuf, osem):
    rows = jnp.concatenate([rows_ref[k].reshape(TX * C, LANES) for k in range(GY)], axis=1)
    gain, shift = affine_ref[0], affine_ref[1]

    def group(i, carry):
        for p in range(2):
            y = 4 * i + 2 * p
            table = table_ref[pl.ds(pl.multiple_of(y * N, 2 * N), 2 * N), :]
            both = lax.dot_general(
                rows, table, (((1,), (1,)), ((), ())), preferred_element_type=F32
            )
            for j in range(2):
                value = both[:, j * N : (j + 1) * N].reshape(TX, C, N) + skip_ref[y + j]
                spread = jnp.mean(value * value, axis=1, keepdims=True)
                value = value * lax.rsqrt(spread + NORM_EPS) * gain[None] + shift[None]
                value = value * (lax.erf(value * math.sqrt(0.5)) + 1.0) * 0.5
                obuf[:, y + j] = value.astype(BF16)
        pltpu.make_async_copy(
            obuf.at[:, pl.ds(4 * i, 4)], out_hbm.at[:, pl.ds(4 * i, 4)], osem.at[i]
        ).start()
        return carry

    lax.fori_loop(0, TY // 4, group, 0)
    for i in range(TY // 4):
        pltpu.make_async_copy(
            obuf.at[:, pl.ds(4 * i, 4)], out_hbm.at[:, pl.ds(4 * i, 4)], osem.at[i]
        ).wait()


def local(fields, spectral, skip_weight, skip_bias, norm_gain, norm_shift):
    weights = jnp.transpose(spectral[0, 0], (0, 1, 3, 4, 2))
    params = jnp.concatenate([skip_bias, norm_gain, norm_shift], axis=0)
    dma = pltpu.SemaphoreType.DMA
    anywhere = pl.BlockSpec(memory_space=pltpu.HBM)
    vmem = pl.BlockSpec(memory_space=pltpu.VMEM)
    far_x = len(FAR_X)
    rows, table, skip, affine = pl.pallas_call(
        modes_kernel,
        name="modes",
        out_shape=[
            pltpu.VMEM((GY, TX, C, LANES), BF16),
            pltpu.VMEM((TY * N, PEER), BF16),
            pltpu.VMEM((TY, TX, C, N), F32),
            pltpu.VMEM((2, C, N), F32),
        ],
        in_specs=[anywhere] * 7,
        out_specs=[vmem] * 4,
        scratch_shapes=[
            pltpu.VMEM((TX, TY, C, N), BF16),
            pltpu.VMEM((KY, 2, C // COL, M, C), BF16),
            pltpu.VMEM((C, C), BF16),
            pltpu.VMEM((3, C), F32),
            pltpu.VMEM((2, N, LANES), F32),
            pltpu.VMEM((2 * TY * GY, LANES), F32),
            pltpu.VMEM((2 * 9 * TX, LANES), F32),
            pltpu.VMEM((GY, 2, TX, HALF, LANES), BF16),
            pltpu.VMEM((3, 2, TX, HALF, LANES), BF16),
            pltpu.VMEM((2, M, HALF, LANES), BF16),
            pltpu.VMEM((far_x, 2, HALF, LANES), BF16),
            pltpu.VMEM((C, LANES), F32),
            pltpu.VMEM((C, LANES), F32),
            pltpu.VMEM((COL, C // COL, C, LANES), BF16),
            pltpu.VMEM((GX, 2, HALF, LANES), BF16),
            dma((4,)), dma((6,)),
            dma((3, 2)), dma((3, 2)),
            dma((far_x, 2)), dma((far_x, 2)),
            dma((far_x, 2)), dma((far_x, 2)),
            dma((3, 2)), dma((3, 2)),
            dma((3,)), dma((3,)),
            dma((4,)), dma((4,)),
        ],
        compiler_params=pltpu.CompilerParams(
            collective_id=0, has_side_effects=True, vmem_limit_bytes=48 << 20
        ),
    )(
        fields[0], weights, skip_weight[0], params,
        jnp.asarray(base_tables()), jnp.asarray(turn_tables()), jnp.asarray(first_tables()),
    )
    out = pl.pallas_call(
        finish_kernel,
        name="finish",
        out_shape=jax.ShapeDtypeStruct((TX, TY, C, N), BF16),
        in_specs=[vmem] * 4,
        out_specs=anywhere,
        scratch_shapes=[pltpu.VMEM((TX, TY, C, N), BF16), dma((TY // 4,))],
        compiler_params=pltpu.CompilerParams(vmem_limit_bytes=48 << 20),
    )(rows, table, skip, affine)
    return out[None]


def solution(mesh):
    placed = (
        P("col", "gx", "gy", None, None),
        P(None, "gx", "gy", None, None, "col", None),
        P(),
        P(),
        P(),
        P(),
    )
    return jax.shard_map(
        local,
        mesh=mesh,
        in_specs=placed,
        out_specs=P("col", "gx", "gy", None, None),
        check_vma=False,
    )
```

```python
import functools
import math

import jax
import jax.numpy as jnp
import numpy as np
from jax import lax
from jax.experimental import pallas as pl
from jax.experimental.pallas import tpu as pltpu
from jax.sharding import PartitionSpec as P

MESH = pl.DeviceIdType.MESH
F32, BF16 = jnp.float32, jnp.bfloat16

N = 128
M = 16
C = 32
GX, GY, COL = 16, 4, 8
TX, TY = N // GX, N // GY
KY = M // GY
LANES = 2 * KY * M
PEER = GY * LANES
HALF = C // 2
NORM_EPS = 1e-05

FAR_X = [(dy, dz) for dz in (4, 3, 5, 2, 6, 1, 7, 0) for dy in (1, 0) if (dy, dz) != (0, 0)]
FAR_Y = (2, 1, 3)
FAR_COL = (2, 1, 3)
SKIP_EARLY = 4


def signed(k):
    return np.where(k < M // 2, k, k - M)


def base_tables():
    turn = np.outer(np.arange(N), np.arange(M)) % N * (2.0 * math.pi / N)
    cosine, sine = np.tile(np.cos(turn), (1, KY)), np.tile(np.sin(turn), (1, KY))
    first = np.concatenate([cosine, -sine], axis=1)
    second = np.concatenate([-sine, -cosine], axis=1)
    return np.stack([first, second]).astype(np.float32)


def turn_tables():
    out = np.zeros((GY, 2, TY, GY, LANES), np.float32)
    for g in range(GY):
        for step in range(GY):
            ky = (g + step) % GY * KY + np.arange(KY)
            turn = np.outer(g * TY + np.arange(TY), signed(ky)) % N * (2.0 * math.pi / N)
            out[g, 0, :, step] = np.tile(np.repeat(np.cos(turn), M, axis=1), (1, 2))
            out[g, 1, :, step] = np.tile(np.repeat(np.sin(turn), M, axis=1), (1, 2))
    return out.reshape(GY, 2 * TY * GY, LANES)


def first_tables():
    f = np.arange(M // 2 + 1)
    out = np.zeros((GX, 2, f.size, TX), np.float32)
    for g in range(GX):
        turn = np.outer(f, g * TX + np.arange(TX)) % N * (2.0 * math.pi / N)
        out[g, 0], out[g, 1] = np.cos(turn), np.sin(turn)
    out = out.reshape(GX, -1, 1)
    return np.ascontiguousarray(np.broadcast_to(out, (GX, out.shape[1], LANES)))


def turned(v):
    lane = lax.broadcasted_iota(jnp.int32, v.shape, v.ndim - 1)
    swapped = pltpu.roll(v, LANES // 2, v.ndim - 1)
    return jnp.where(lane < LANES // 2, swapped, -swapped)


def modes_kernel(
    h_hbm, w_hbm, skw_hbm, bias_hbm, gain_hbm, shift_hbm, base_hbm, turn_hbm, first_hbm,
    rows_ref, table_ref, skip_ref, affine_ref,
    hbuf, wraw, skw, par, base, turn, first,
    zsend, arecv, pm, brecv, spec, mixf, wbuf, mrecv,
    lsem, asend, arcv, bsend, brcv, csend, crcv, dsend, drcv, wsend, wrcv, vsend, vrcv,
):
    gx, gy, col = lax.axis_index("gx"), lax.axis_index("gy"), lax.axis_index("col")
    y_lo, z = gx // 8, gx % 8
    y_hi, core = col // 2, col % 2
    sibling = col + 1 - 2 * core

    def x_peer(dy, dz):
        return (y_lo + dy) % 2 * 8 + (z + dz) % 8

    tables = [
        pltpu.make_async_copy(base_hbm, base, lsem.at[0]),
        pltpu.make_async_copy(turn_hbm.at[gy], turn, lsem.at[1]),
    ]
    cells_in = pltpu.make_async_copy(h_hbm, hbuf, lsem.at[2])
    weights_in = pltpu.make_async_copy(w_hbm, wraw, lsem.at[3])
    loads = [
        pltpu.make_async_copy(skw_hbm, skw, lsem.at[4]),
        pltpu.make_async_copy(bias_hbm, par.at[0], lsem.at[5]),
        pltpu.make_async_copy(gain_hbm, par.at[1], lsem.at[6]),
        pltpu.make_async_copy(shift_hbm, par.at[2], lsem.at[7]),
        pltpu.make_async_copy(first_hbm.at[gx], first, lsem.at[8]),
    ]
    for cp in [*tables, cells_in, weights_in, *loads]:
        cp.start()

    def landed(ref, sem):
        pltpu.make_async_copy(ref, ref, sem).wait()

    barrier = pltpu.get_barrier_semaphore()
    for dy, dz in FAR_X:
        pl.semaphore_signal(barrier, 1, device_id={"gx": x_peer(dy, dz)}, device_id_type=MESH)
    for k in FAR_Y:
        pl.semaphore_signal(barrier, 1, device_id={"gy": (gy + k) % GY}, device_id_type=MESH)
    for k in FAR_COL:
        pl.semaphore_signal(
            barrier, 1, device_id={"col": (y_hi + k) % 4 * 2 + core}, device_id_type=MESH
        )
    pl.semaphore_signal(barrier, 1, device_id={"col": sibling}, device_id_type=MESH)

    for cp in tables:
        cp.wait()

    def table_row(y, carry):
        for k in range(GY):
            cosine = turn[pl.ds(y * GY + k, 1), :]
            sine = turn[pl.ds(TY * GY + y * GY + k, 1), :]
            table_ref[pl.ds(pl.multiple_of(y * N, N), N), k * LANES : (k + 1) * LANES] = (
                base[0] * cosine + base[1] * sine
            ).astype(BF16)
        return carry

    lax.fori_loop(0, TY, table_row, 0)
    cells_in.wait()
    cells = jnp.concatenate([hbuf[:, y].reshape(TX * C, N) for y in range(TY)], axis=1)
    local = jnp.dot(cells, table_ref[...], preferred_element_type=F32)
    for k in range(GY):
        part = local[:, k * LANES : (k + 1) * LANES].astype(BF16).reshape(TX, 2, HALF, LANES)
        for half in range(2):
            zsend[k, half] = part[:, half]

    pl.semaphore_wait(barrier, len(FAR_X) + len(FAR_Y) + len(FAR_COL) + 1)

    for half in range(2):
        for k in FAR_Y:
            pltpu.make_async_remote_copy(
                zsend.at[k, half], arecv.at[half, k - 1], asend.at[0], arcv.at[half],
                device_id={"gy": (gy + k) % GY}, device_id_type=MESH,
            ).start()

    weights_in.wait()
    for d in range(C // COL):
        block = jnp.concatenate(
            [wraw[k, s, d].astype(F32) for s in range(2) for k in range(KY)], axis=0
        )
        wbuf[col, d] = block.T.astype(BF16)
    for k in FAR_COL:
        pltpu.make_async_remote_copy(
            wbuf.at[col], wbuf.at[col], wsend.at[0], wrcv.at[0],
            device_id={"col": (y_hi + k) % 4 * 2 + core}, device_id_type=MESH,
        ).start()

    def to_sibling(slot):
        pltpu.make_async_remote_copy(
            wbuf.at[slot], wbuf.at[slot], vsend.at[0], vrcv.at[0],
            device_id={"col": sibling}, device_id_type=MESH,
        ).start()

    to_sibling(col)

    for cp in loads:
        cp.wait()
    wide = [jnp.broadcast_to(par[i], (N, C)).T for i in range(3)]
    affine_ref[0] = wide[1] * math.sqrt(0.5 * C)
    affine_ref[1] = wide[2] * math.sqrt(0.5)
    bias = wide[0] - jnp.mean(wide[0], axis=0, keepdims=True)
    pick = (
        lax.broadcasted_iota(jnp.int32, (C, TX * C), 1) % C
        == lax.broadcasted_iota(jnp.int32, (C, TX * C), 0)
    )
    spread = jnp.dot(skw[...], pick.astype(F32).astype(BF16), preferred_element_type=F32)
    spread = jnp.broadcast_to(spread[None], (TX, C, TX * C)).reshape(TX * C, TX * C)
    same = (
        lax.broadcasted_iota(jnp.int32, (TX * C, TX * C), 0) // C
        == lax.broadcasted_iota(jnp.int32, (TX * C, TX * C), 1) // C
    )
    diagonal = jnp.where(same, spread, 0.0).astype(BF16)

    def skip_rows(i, carry):
        four = [hbuf[:, 4 * i + j].reshape(TX * C, N) for j in range(4)]
        out = jnp.dot(diagonal, jnp.concatenate(four, axis=1), preferred_element_type=F32)
        for j in range(4):
            value = out[:, j * N : (j + 1) * N].reshape(TX, C, N)
            value = value - jnp.mean(value, axis=1, keepdims=True) + bias[None]
            skip_ref[4 * i + j] = value
        return carry

    lax.fori_loop(0, SKIP_EARLY, skip_rows, 0)

    for half in range(2):
        landed(arecv.at[half], arcv.at[half])
        here, there = [], []
        for x in range(TX):
            v = zsend[0, half, x].astype(F32)
            for k in range(3):
                v = v + arecv[half, k, x].astype(F32)
            here.append(v)
            there.append(turned(v))
        for f in range(M // 2 + 1):
            even = odd = None
            for x in range(TX):
                if f == 0:
                    even = here[x] if even is None else even + here[x]
                    continue
                r = f * TX + x
                a = here[x] * first[r : r + 1, :]
                b = there[x] * first[9 * TX + r : 9 * TX + r + 1, :]
                even = a if even is None else even + a
                odd = b if odd is None else odd + b
            if f == 0:
                pm[half, 0] = even.astype(BF16)
                continue
            if f < M // 2:
                pm[half, f] = (even + odd).astype(BF16)
            pm[half, M - f] = (even - odd).astype(BF16)
        for i, (dy, dz) in enumerate(FAR_X):
            to = x_peer(dy, dz)
            pltpu.make_async_remote_copy(
                pm.at[half, to], brecv.at[half, i], bsend.at[0], brcv.at[half],
                device_id={"gx": to}, device_id_type=MESH,
            ).start()

    lax.fori_loop(SKIP_EARLY, TY // 4, skip_rows, 0)

    landed(wbuf.at[0:3], wrcv.at[0])
    for k in FAR_COL:
        to_sibling((y_hi + 4 - k) % 4 * 2 + core)

    scale = 1.0 / math.sqrt(N * N * N)
    for half in range(2):
        total = pm[half, gx].astype(F32)
        landed(brecv.at[half], brcv.at[half])
        for i in range(len(FAR_X)):
            total = total + brecv[half, i].astype(F32)
        spec[half * HALF : (half + 1) * HALF, :] = (total * scale).astype(BF16).astype(F32)
    landed(wbuf.at[0:4], vrcv.at[0])

    straight = spec[...]
    crossed = pltpu.roll(straight, LANES // 2, 1)
    lane = lax.broadcasted_iota(jnp.int32, (8, LANES), 1)
    for g in range(4):
        weight = wbuf[2 * g : 2 * g + 2].astype(F32).reshape(8, C, LANES)
        a = jnp.sum(weight * straight[None], axis=1)
        b = jnp.sum(weight * crossed[None], axis=1)
        mixed = jnp.where(
            lane < LANES // 2, a - pltpu.roll(a, LANES // 2, 1), b + pltpu.roll(b, LANES // 2, 1)
        )
        mixf[8 * g : 8 * g + 8, :] = mixed
    mixed = mixf[...]
    mixed = (mixed - jnp.mean(mixed, axis=0, keepdims=True)) * (1.0 / math.sqrt(M * M * M))
    mixed = mixed.astype(BF16)

    mrecv[gx] = mixed
    for dy, dz in FAR_X:
        pltpu.make_async_remote_copy(
            mrecv.at[gx], mrecv.at[gx], csend.at[0], crcv.at[0],
            device_id={"gx": x_peer(dy, dz)}, device_id_type=MESH,
        ).start()

    landed(mrecv.at[0 : GX - 1], crcv.at[0])
    for half in range(2):
        part = slice(half * HALF, (half + 1) * HALF)
        zero = mrecv[0, part].astype(F32)
        out = [zero for _ in range(TX)]
        for f in range(1, M // 2 + 1):
            low = mrecv[M - f, part].astype(F32)
            if f < M // 2:
                high = mrecv[f, part].astype(F32)
                even, odd = high + low, turned(low - high)
            else:
                even, odd = low, turned(low)
            for x in range(TX):
                r = f * TX + x
                out[x] = out[x] + even * first[r : r + 1, :]
                out[x] = out[x] + odd * first[9 * TX + r : 9 * TX + r + 1, :]
        for x in range(TX):
            rows_ref[0, x, part, :] = out[x].astype(BF16)
        for k in FAR_Y:
            span = pl.ds(half * HALF, HALF)
            pltpu.make_async_remote_copy(
                rows_ref.at[0, :, span, :], rows_ref.at[k, :, span, :], dsend.at[0], drcv.at[0],
                device_id={"gy": (gy + GY - k) % GY}, device_id_type=MESH,
            ).start()

    landed(zsend.at[1:4], asend.at[0])
    landed(wbuf.at[0:3], wsend.at[0])
    landed(wbuf.at[0:4], vsend.at[0])
    landed(brecv, bsend.at[0])
    landed(mrecv.at[0 : GX - 1], csend.at[0])
    landed(rows_ref.at[1:4], dsend.at[0])
    landed(rows_ref.at[1:4], drcv.at[0])


def finish_kernel(rows_ref, table_ref, skip_ref, affine_ref, out_hbm, obuf, acc, osem):
    rows = jnp.concatenate([rows_ref[k].reshape(TX * C, LANES) for k in range(GY)], axis=1)
    gain, shift = affine_ref[0], affine_ref[1]

    def transform(i, slot):
        for p in range(2):
            y = 4 * i + 2 * p
            table = table_ref[pl.ds(pl.multiple_of(y * N, 2 * N), 2 * N), :]
            both = lax.dot_general(
                rows, table, (((1,), (1,)), ((), ())), preferred_element_type=F32
            )
            for j in range(2):
                acc[slot, 2 * p + j] = both[:, j * N : (j + 1) * N].reshape(TX, C, N)

    def settle(i, slot):
        for j in range(4):
            value = acc[slot, j] + skip_ref[4 * i + j]
            spread = jnp.sum(value * value, axis=1, keepdims=True)
            value = value * lax.rsqrt(spread + C * NORM_EPS) * gain[None] + shift[None]
            value = (value * math.sqrt(0.5)) * (lax.erf(value) + 1.0)
            obuf[:, 4 * i + j] = value.astype(BF16)
        written(i).start()

    def written(i):
        span = pl.ds(4 * i, 4)
        return pltpu.make_async_copy(obuf.at[:, span], out_hbm.at[:, span], osem.at[0])

    transform(0, 0)

    def two(i, carry):
        transform(2 * i + 1, 1)
        settle(2 * i, 0)
        transform(jnp.minimum(2 * i + 2, TY // 4 - 1), 0)
        settle(2 * i + 1, 1)
        return carry

    lax.fori_loop(0, TY // 8, two, 0)
    pltpu.make_async_copy(obuf, out_hbm, osem.at[0]).wait()


def local(fields, spectral, skip_weight, skip_bias, norm_gain, norm_shift):
    weights = jnp.transpose(spectral[0, 0], (0, 1, 3, 4, 2))
    dma = pltpu.SemaphoreType.DMA
    anywhere = pl.BlockSpec(memory_space=pltpu.HBM)
    vmem = pl.BlockSpec(memory_space=pltpu.VMEM)
    far_x = len(FAR_X)
    rows, table, skip, affine = pl.pallas_call(
        modes_kernel,
        name="modes",
        out_shape=[
            pltpu.VMEM((GY, TX, C, LANES), BF16),
            pltpu.VMEM((TY * N, PEER), BF16),
            pltpu.VMEM((TY, TX, C, N), F32),
            pltpu.VMEM((2, C, N), F32),
        ],
        in_specs=[anywhere] * 9,
        out_specs=[vmem] * 4,
        scratch_shapes=[
            pltpu.VMEM((TX, TY, C, N), BF16),
            pltpu.VMEM((KY, 2, C // COL, M, C), BF16),
            pltpu.VMEM((C, C), BF16),
            pltpu.VMEM((3, 1, C), F32),
            pltpu.VMEM((2, N, LANES), F32),
            pltpu.VMEM((2 * TY * GY, LANES), F32),
            pltpu.VMEM((2 * 9 * TX, LANES), F32),
            pltpu.VMEM((GY, 2, TX, HALF, LANES), BF16),
            pltpu.VMEM((2, 3, TX, HALF, LANES), BF16),
            pltpu.VMEM((2, M, HALF, LANES), BF16),
            pltpu.VMEM((2, far_x, HALF, LANES), BF16),
            pltpu.VMEM((C, LANES), F32),
            pltpu.VMEM((C, LANES), F32),
            pltpu.VMEM((COL, C // COL, C, LANES), BF16),
            pltpu.VMEM((GX, C, LANES), BF16),
            dma((9,)),
            dma((1,)), dma((2,)),
            dma((1,)), dma((2,)),
            dma((1,)), dma((1,)),
            dma((1,)), dma((1,)),
            dma((1,)), dma((1,)),
            dma((1,)), dma((1,)),
        ],
        compiler_params=pltpu.CompilerParams(
            collective_id=0, has_side_effects=True, vmem_limit_bytes=48 << 20
        ),
    )(
        fields[0], weights, skip_weight[0], skip_bias, norm_gain, norm_shift,
        jnp.asarray(base_tables()), jnp.asarray(turn_tables()), jnp.asarray(first_tables()),
    )
    out = pl.pallas_call(
        finish_kernel,
        name="finish",
        out_shape=jax.ShapeDtypeStruct((TX, TY, C, N), BF16),
        in_specs=[vmem] * 4,
        out_specs=anywhere,
        scratch_shapes=[
            pltpu.VMEM((TX, TY, C, N), BF16),
            pltpu.VMEM((2, 4, TX, C, N), F32),
            dma((1,)),
        ],
        compiler_params=pltpu.CompilerParams(vmem_limit_bytes=16 << 20),
    )(rows, table, skip, affine)
    return out[None]


def solution(mesh):
    placed = (
        P("col", "gx", "gy", None, None),
        P(None, "gx", "gy", None, None, "col", None),
        P(),
        P(),
        P(),
        P(),
    )
    return jax.shard_map(
        local,
        mesh=mesh,
        in_specs=placed,
        out_specs=P("col", "gx", "gy", None, None),
        check_vma=False,
    )
```

```python
import functools
import math

import jax
import jax.numpy as jnp
import numpy as np
from jax import lax
from jax.experimental import pallas as pl
from jax.experimental.pallas import tpu as pltpu
from jax.sharding import PartitionSpec as P

MESH = pl.DeviceIdType.MESH
F32, BF16 = jnp.float32, jnp.bfloat16

N = 128
M = 16
C = 32
GX, GY, COL = 16, 4, 8
TX, TY = N // GX, N // GY
KY = M // GY
LANES = 2 * KY * M
PEER = GY * LANES
HALF = C // 2
XH = TX // 2
NORM_EPS = 1e-05

FAR_X = [(dy, dz) for dz in (4, 3, 5, 2, 6, 1, 7, 0) for dy in (1, 0) if (dy, dz) != (0, 0)]
FAR_Y = (2, 1, 3)
FAR_COL = (2, 1, 3)
EARLY_ROWS = 14
WRITE = 4


def signed(k):
    return np.where(k < M // 2, k, k - M)


def base_tables():
    turn = np.outer(np.arange(N), np.arange(M)) % N * (2.0 * math.pi / N)
    cosine, sine = np.tile(np.cos(turn), (1, KY)), np.tile(np.sin(turn), (1, KY))
    first = np.concatenate([cosine, -sine], axis=1)
    second = np.concatenate([-sine, -cosine], axis=1)
    return np.stack([first, second]).astype(np.float32)


def turn_tables():
    out = np.zeros((GY, 2, TY, GY, LANES), np.float32)
    for g in range(GY):
        for step in range(GY):
            ky = (g + step) % GY * KY + np.arange(KY)
            turn = np.outer(g * TY + np.arange(TY), signed(ky)) % N * (2.0 * math.pi / N)
            out[g, 0, :, step] = np.tile(np.repeat(np.cos(turn), M, axis=1), (1, 2))
            out[g, 1, :, step] = np.tile(np.repeat(np.sin(turn), M, axis=1), (1, 2))
    return out.reshape(GY, 2 * TY * GY, LANES)


def first_tables():
    f = np.arange(M // 2 + 1)
    out = np.zeros((GX, 2, f.size, TX), np.float32)
    for g in range(GX):
        turn = np.outer(f, g * TX + np.arange(TX)) % N * (2.0 * math.pi / N)
        out[g, 0], out[g, 1] = np.cos(turn), np.sin(turn)
    out = out.reshape(GX, -1, 1)
    return np.ascontiguousarray(np.broadcast_to(out, (GX, out.shape[1], LANES)))


def turned(v):
    lane = lax.broadcasted_iota(jnp.int32, v.shape, v.ndim - 1)
    swapped = pltpu.roll(v, LANES // 2, v.ndim - 1)
    return jnp.where(lane < LANES // 2, swapped, -swapped)


def modes_kernel(
    h_hbm, w_hbm, skw_hbm, bias_hbm, gain_hbm, shift_hbm, base_hbm, turn_hbm, first_hbm,
    rows_late, back_ref, skip_late, affine_ref, out_early,
    rows_early, skip_early, table, hbuf, wraw, skw, par, base, turn, first,
    zsend, arecv, pm, brecv, spec, mixf, wbuf, mrecv,
    lsem, asend, arcv, bsend, brcv, csend, crcv, dsend, drcv, wsend, wrcv, vsend, vrcv,
):
    gx, gy, col = lax.axis_index("gx"), lax.axis_index("gy"), lax.axis_index("col")
    y_lo, z = gx // 8, gx % 8
    y_hi, core = col // 2, col % 2
    sibling = col + 1 - 2 * core

    def x_peer(dy, dz):
        return (y_lo + dy) % 2 * 8 + (z + dz) % 8

    tables = [
        pltpu.make_async_copy(base_hbm, base, lsem.at[0]),
        pltpu.make_async_copy(turn_hbm.at[gy], turn, lsem.at[1]),
    ]
    cells_in = pltpu.make_async_copy(h_hbm, hbuf, lsem.at[2])
    weights_in = pltpu.make_async_copy(w_hbm, wraw, lsem.at[3])
    loads = [
        pltpu.make_async_copy(skw_hbm, skw, lsem.at[4]),
        pltpu.make_async_copy(bias_hbm, par.at[0], lsem.at[5]),
        pltpu.make_async_copy(gain_hbm, par.at[1], lsem.at[6]),
        pltpu.make_async_copy(shift_hbm, par.at[2], lsem.at[7]),
        pltpu.make_async_copy(first_hbm.at[gx], first, lsem.at[8]),
    ]
    for cp in [*tables, cells_in, weights_in, *loads]:
        cp.start()

    def landed(ref, sem):
        pltpu.make_async_copy(ref, ref, sem).wait()

    barrier = pltpu.get_barrier_semaphore()
    for dy, dz in FAR_X:
        pl.semaphore_signal(barrier, 1, device_id={"gx": x_peer(dy, dz)}, device_id_type=MESH)
    for k in FAR_Y:
        pl.semaphore_signal(barrier, 1, device_id={"gy": (gy + k) % GY}, device_id_type=MESH)
    for k in FAR_COL:
        pl.semaphore_signal(
            barrier, 1, device_id={"col": (y_hi + k) % 4 * 2 + core}, device_id_type=MESH
        )
    pl.semaphore_signal(barrier, 1, device_id={"col": sibling}, device_id_type=MESH)

    for cp in tables:
        cp.wait()

    def table_row(y):
        for k in range(GY):
            cosine = turn[y * GY + k : y * GY + k + 1, :]
            sine = turn[(TY + y) * GY + k : (TY + y) * GY + k + 1, :]
            table[y, k] = (base[0] * cosine + base[1] * sine).astype(BF16)

    for y in range(EARLY_ROWS):
        table_row(y)
    cells_in.wait()
    for y in range(EARLY_ROWS, TY):
        table_row(y)
    cells = jnp.concatenate([hbuf[:, y].reshape(TX * C, N) for y in range(TY)], axis=1)
    steps = [table[:, k].reshape(TY * N, LANES) for k in range(GY)]
    local = jnp.dot(cells, jnp.concatenate(steps, axis=1), preferred_element_type=F32)
    for k in range(GY):
        part = local[:, k * LANES : (k + 1) * LANES].astype(BF16).reshape(TX, 2, HALF, LANES)
        for half in range(2):
            zsend[k, half] = part[:, half]

    pl.semaphore_wait(barrier, len(FAR_X) + len(FAR_Y) + len(FAR_COL) + 1)

    for half in range(2):
        for k in FAR_Y:
            pltpu.make_async_remote_copy(
                zsend.at[k, half], arecv.at[half, k - 1], asend.at[0], arcv.at[half],
                device_id={"gy": (gy + k) % GY}, device_id_type=MESH,
            ).start()

    weights_in.wait()
    for d in range(C // COL):
        block = jnp.concatenate(
            [wraw[k, s, d].astype(F32) for s in range(2) for k in range(KY)], axis=0
        )
        wbuf[col, d] = block.T.astype(BF16)
    for k in FAR_COL:
        pltpu.make_async_remote_copy(
            wbuf.at[col], wbuf.at[col], wsend.at[0], wrcv.at[0],
            device_id={"col": (y_hi + k) % 4 * 2 + core}, device_id_type=MESH,
        ).start()

    def to_sibling(slot):
        pltpu.make_async_remote_copy(
            wbuf.at[slot], wbuf.at[slot], vsend.at[0], vrcv.at[0],
            device_id={"col": sibling}, device_id_type=MESH,
        ).start()

    to_sibling(col)

    for cp in loads:
        cp.wait()
    wide = [jnp.broadcast_to(par[i], (N, C)).T for i in range(3)]
    affine_ref[0] = wide[1] * math.sqrt(0.5 * C)
    affine_ref[1] = wide[2] * math.sqrt(0.5)
    bias = wide[0] - jnp.mean(wide[0], axis=0, keepdims=True)
    pick = (
        lax.broadcasted_iota(jnp.int32, (C, TX * C), 1) % C
        == lax.broadcasted_iota(jnp.int32, (C, TX * C), 0)
    )
    spread = jnp.dot(skw[...], pick.astype(F32).astype(BF16), preferred_element_type=F32)
    spread = jnp.broadcast_to(spread[None], (TX, C, TX * C)).reshape(TX * C, TX * C)
    same = (
        lax.broadcasted_iota(jnp.int32, (TX * C, TX * C), 0) // C
        == lax.broadcasted_iota(jnp.int32, (TX * C, TX * C), 1) // C
    )
    diagonal = jnp.where(same, spread, 0.0).astype(BF16)

    def skip_rows(i, carry):
        four = [hbuf[:, 4 * i + j].reshape(TX * C, N) for j in range(4)]
        out = jnp.dot(diagonal, jnp.concatenate(four, axis=1), preferred_element_type=F32)
        for j in range(4):
            value = out[:, j * N : (j + 1) * N].reshape(TX, C, N)
            value = value - jnp.mean(value, axis=1, keepdims=True) + bias[None]
            skip_early[4 * i + j] = value[:XH]
            skip_late[4 * i + j] = value[XH:]
        return carry

    lax.fori_loop(0, TY // 4, skip_rows, 0)

    for half in range(2):
        landed(arecv.at[half], arcv.at[half])
        here, there = [], []
        for x in range(TX):
            v = zsend[0, half, x].astype(F32)
            for k in range(3):
                v = v + arecv[half, k, x].astype(F32)
            here.append(v)
            there.append(turned(v))
        for f in range(M // 2 + 1):
            even = odd = None
            for x in range(TX):
                if f == 0:
                    even = here[x] if even is None else even + here[x]
                    continue
                r = f * TX + x
                a = here[x] * first[r : r + 1, :]
                b = there[x] * first[9 * TX + r : 9 * TX + r + 1, :]
                even = a if even is None else even + a
                odd = b if odd is None else odd + b
            if f == 0:
                pm[half, 0] = even.astype(BF16)
                continue
            if f < M // 2:
                pm[half, f] = (even + odd).astype(BF16)
            pm[half, M - f] = (even - odd).astype(BF16)
        for i, (dy, dz) in enumerate(FAR_X):
            to = x_peer(dy, dz)
            pltpu.make_async_remote_copy(
                pm.at[half, to], brecv.at[half, i], bsend.at[0], brcv.at[half],
                device_id={"gx": to}, device_id_type=MESH,
            ).start()

    landed(wbuf.at[0:3], wrcv.at[0])
    for k in FAR_COL:
        to_sibling((y_hi + 4 - k) % 4 * 2 + core)

    scale = 1.0 / math.sqrt(N * N * N)
    for half in range(2):
        total = pm[half, gx].astype(F32)
        landed(brecv.at[half], brcv.at[half])
        for i in range(len(FAR_X)):
            total = total + brecv[half, i].astype(F32)
        spec[half * HALF : (half + 1) * HALF, :] = (total * scale).astype(BF16).astype(F32)
    landed(wbuf.at[0:4], vrcv.at[0])

    straight = spec[...]
    crossed = pltpu.roll(straight, LANES // 2, 1)
    lane = lax.broadcasted_iota(jnp.int32, (8, LANES), 1)
    for g in range(4):
        weight = wbuf[2 * g : 2 * g + 2].astype(F32).reshape(8, C, LANES)
        a = jnp.sum(weight * straight[None], axis=1)
        b = jnp.sum(weight * crossed[None], axis=1)
        mixed = jnp.where(
            lane < LANES // 2, a - pltpu.roll(a, LANES // 2, 1), b + pltpu.roll(b, LANES // 2, 1)
        )
        mixf[8 * g : 8 * g + 8, :] = mixed
    mixed = mixf[...]
    mixed = (mixed - jnp.mean(mixed, axis=0, keepdims=True)) * (1.0 / math.sqrt(M * M * M))
    mixed = mixed.astype(BF16)

    mrecv[gx] = mixed
    for dy, dz in FAR_X:
        pltpu.make_async_remote_copy(
            mrecv.at[gx], mrecv.at[gx], csend.at[0], crcv.at[0],
            device_id={"gx": x_peer(dy, dz)}, device_id_type=MESH,
        ).start()

    def table_column(y, carry):
        for k in range(GY):
            back_ref[y, k] = table[y, k].T
        return carry

    lax.fori_loop(0, TY, table_column, 0)

    landed(mrecv.at[0 : GX - 1], crcv.at[0])
    for late, rows in enumerate((rows_early, rows_late)):
        for half in range(2):
            part = slice(half * HALF, (half + 1) * HALF)
            zero = mrecv[0, part].astype(F32)
            out = [zero for _ in range(XH)]
            for f in range(1, M // 2 + 1):
                low = mrecv[M - f, part].astype(F32)
                if f < M // 2:
                    high = mrecv[f, part].astype(F32)
                    even, odd = high + low, turned(low - high)
                else:
                    even, odd = low, turned(low)
                for x in range(XH):
                    r = f * TX + late * XH + x
                    out[x] = out[x] + even * first[r : r + 1, :]
                    out[x] = out[x] + odd * first[9 * TX + r : 9 * TX + r + 1, :]
            for x in range(XH):
                rows[0, x, part, :] = out[x].astype(BF16)
        for k in FAR_Y:
            pltpu.make_async_remote_copy(
                rows.at[0], rows.at[k], dsend.at[0], drcv.at[late],
                device_id={"gy": (gy + GY - k) % GY}, device_id_type=MESH,
            ).start()

    landed(rows_early.at[1:4], drcv.at[0])
    settle(rows_early, back_ref, skip_early, affine_ref, out_early)

    landed(zsend.at[1:4], asend.at[0])
    landed(wbuf.at[0:3], wsend.at[0])
    landed(wbuf.at[0:4], vsend.at[0])
    landed(brecv, bsend.at[0])
    landed(mrecv.at[0 : GX - 1], csend.at[0])
    landed(zsend.at[1:4], dsend.at[0])
    landed(rows_late.at[1:4], drcv.at[1])


def settle(rows_ref, back_ref, skip_ref, affine_ref, out_ref, written=None):
    rows = jnp.concatenate([rows_ref[k].reshape(XH * C, LANES) for k in range(GY)], axis=1)
    for y in range(0, TY, 2):
        back = [back_ref[y + j].reshape(PEER, N) for j in range(2)]
        both = jnp.dot(rows, jnp.concatenate(back, axis=1), preferred_element_type=F32)
        for j in range(2):
            for x in range(XH):
                value = both[x * C : (x + 1) * C, j * N : (j + 1) * N] + skip_ref[y + j, x]
                spread = jnp.sum(value * value, axis=0, keepdims=True)
                value = value * lax.rsqrt(spread + C * NORM_EPS) * affine_ref[0] + affine_ref[1]
                value = (value * math.sqrt(0.5)) * (lax.erf(value) + 1.0)
                out_ref[x, y + j] = value.astype(BF16)
        if written is not None and y % WRITE == WRITE - 2:
            written(pl.ds(y + 2 - WRITE, WRITE))


def finish_kernel(
    rows_late, back_ref, skip_late, affine_ref, out_early, out_hbm, out_late, early_sem, late_sem
):
    early = pltpu.make_async_copy(out_early, out_hbm.at[0:XH], early_sem.at[0])
    early.start()

    def written(span):
        pltpu.make_async_copy(
            out_late.at[:, span], out_hbm.at[XH:TX, span], late_sem.at[0]
        ).start()

    settle(rows_late, back_ref, skip_late, affine_ref, out_late, written)
    early.wait()
    pltpu.make_async_copy(out_late, out_hbm.at[XH:TX], late_sem.at[0]).wait()


def local(fields, spectral, skip_weight, skip_bias, norm_gain, norm_shift):
    weights = jnp.transpose(spectral[0, 0], (0, 1, 3, 4, 2))
    dma = pltpu.SemaphoreType.DMA
    anywhere = pl.BlockSpec(memory_space=pltpu.HBM)
    vmem = pl.BlockSpec(memory_space=pltpu.VMEM)
    far_x = len(FAR_X)
    rows, back, skip, affine, early = pl.pallas_call(
        modes_kernel,
        name="modes",
        out_shape=[
            pltpu.VMEM((GY, XH, C, LANES), BF16),
            pltpu.VMEM((TY, GY, LANES, N), BF16),
            pltpu.VMEM((TY, XH, C, N), F32),
            pltpu.VMEM((2, C, N), F32),
            pltpu.VMEM((XH, TY, C, N), BF16),
        ],
        in_specs=[anywhere] * 9,
        out_specs=[vmem] * 5,
        scratch_shapes=[
            pltpu.VMEM((GY, XH, C, LANES), BF16),
            pltpu.VMEM((TY, XH, C, N), F32),
            pltpu.VMEM((TY, GY, N, LANES), BF16),
            pltpu.VMEM((TX, TY, C, N), BF16),
            pltpu.VMEM((KY, 2, C // COL, M, C), BF16),
            pltpu.VMEM((C, C), BF16),
            pltpu.VMEM((3, 1, C), F32),
            pltpu.VMEM((2, N, LANES), F32),
            pltpu.VMEM((2 * TY * GY, LANES), F32),
            pltpu.VMEM((2 * 9 * TX, LANES), F32),
            pltpu.VMEM((GY, 2, TX, HALF, LANES), BF16),
            pltpu.VMEM((2, 3, TX, HALF, LANES), BF16),
            pltpu.VMEM((2, M, HALF, LANES), BF16),
            pltpu.VMEM((2, far_x, HALF, LANES), BF16),
            pltpu.VMEM((C, LANES), F32),
            pltpu.VMEM((C, LANES), F32),
            pltpu.VMEM((COL, C // COL, C, LANES), BF16),
            pltpu.VMEM((GX, C, LANES), BF16),
            dma((9,)),
            dma((1,)), dma((2,)),
            dma((1,)), dma((2,)),
            dma((1,)), dma((1,)),
            dma((1,)), dma((2,)),
            dma((1,)), dma((1,)),
            dma((1,)), dma((1,)),
        ],
        compiler_params=pltpu.CompilerParams(
            collective_id=0, has_side_effects=True, vmem_limit_bytes=48 << 20
        ),
    )(
        fields[0], weights, skip_weight[0], skip_bias, norm_gain, norm_shift,
        jnp.asarray(base_tables()), jnp.asarray(turn_tables()), jnp.asarray(first_tables()),
    )
    out = pl.pallas_call(
        finish_kernel,
        name="finish",
        out_shape=jax.ShapeDtypeStruct((TX, TY, C, N), BF16),
        in_specs=[vmem] * 5,
        out_specs=anywhere,
        scratch_shapes=[pltpu.VMEM((XH, TY, C, N), BF16), dma((1,)), dma((1,))],
        compiler_params=pltpu.CompilerParams(vmem_limit_bytes=16 << 20),
    )(rows, back, skip, affine, early)
    return out[None]


def solution(mesh):
    placed = (
        P("col", "gx", "gy", None, None),
        P(None, "gx", "gy", None, None, "col", None),
        P(),
        P(),
        P(),
        P(),
    )
    return jax.shard_map(
        local,
        mesh=mesh,
        in_specs=placed,
        out_specs=P("col", "gx", "gy", None, None),
        check_vma=False,
    )
```

```python
import functools
import math

import jax
import jax.numpy as jnp
import numpy as np
from jax import lax
from jax.experimental import pallas as pl
from jax.experimental.pallas import tpu as pltpu
from jax.sharding import PartitionSpec as P

MESH = pl.DeviceIdType.MESH
F32, BF16 = jnp.float32, jnp.bfloat16

N = 128
M = 16
C = 32
GX, GY, COL = 16, 4, 8
TX, TY = N // GX, N // GY
KY = M // GY
LANES = 2 * KY * M
PEER = GY * LANES
HALF = C // 2
XH = TX // 2
NORM_EPS = 1e-05

FAR_X = [(dy, dz) for dy in (1, 0) for dz in (4, 3, 5, 2, 6, 1, 7, 0) if (dy, dz) != (0, 0)]
FAR_Y = (2, 1, 3)
FAR_COL = (2, 1, 3)
EARLY_ROWS = 14
WRITE = 4


def signed(k):
    return np.where(k < M // 2, k, k - M)


def base_tables():
    turn = np.outer(np.arange(N), np.arange(M)) % N * (2.0 * math.pi / N)
    cosine, sine = np.tile(np.cos(turn), (1, KY)), np.tile(np.sin(turn), (1, KY))
    first = np.concatenate([cosine, -sine], axis=1)
    second = np.concatenate([-sine, -cosine], axis=1)
    return np.stack([first, second]).astype(np.float32)


def turn_tables():
    out = np.zeros((GY, 2, TY, GY, LANES), np.float32)
    for g in range(GY):
        for step in range(GY):
            ky = (g + step) % GY * KY + np.arange(KY)
            turn = np.outer(g * TY + np.arange(TY), signed(ky)) % N * (2.0 * math.pi / N)
            out[g, 0, :, step] = np.tile(np.repeat(np.cos(turn), M, axis=1), (1, 2))
            out[g, 1, :, step] = np.tile(np.repeat(np.sin(turn), M, axis=1), (1, 2))
    return out.reshape(GY, 2 * TY * GY, LANES)


def first_tables():
    f = np.arange(M // 2 + 1)
    out = np.zeros((GX, 2, f.size, TX), np.float32)
    for g in range(GX):
        turn = np.outer(f, g * TX + np.arange(TX)) % N * (2.0 * math.pi / N)
        out[g, 0], out[g, 1] = np.cos(turn), np.sin(turn)
    out = out.reshape(GX, -1, 1)
    return np.ascontiguousarray(np.broadcast_to(out, (GX, out.shape[1], LANES)))


def turned(v):
    lane = lax.broadcasted_iota(jnp.int32, v.shape, v.ndim - 1)
    swapped = pltpu.roll(v, LANES // 2, v.ndim - 1)
    return jnp.where(lane < LANES // 2, swapped, -swapped)


def modes_kernel(
    h_hbm, w_hbm, skw_hbm, bias_hbm, gain_hbm, shift_hbm, base_hbm, turn_hbm, first_hbm,
    rows_late, back_ref, skip_late, affine_ref, out_early,
    rows_early, skip_early, table, hbuf, wraw, skw, par, base, turn, first,
    zsend, arecv, pm, brecv, spec, mixf, wbuf, mrecv,
    lsem, asend, arcv, bsend, brcv, csend, crcv, dsend, drcv, wsend, wrcv, vsend, vrcv,
):
    gx, gy, col = lax.axis_index("gx"), lax.axis_index("gy"), lax.axis_index("col")
    y_lo, z = gx // 8, gx % 8
    y_hi, core = col // 2, col % 2
    sibling = col + 1 - 2 * core

    def x_peer(dy, dz):
        return (y_lo + dy) % 2 * 8 + (z + dz) % 8

    tables = [
        pltpu.make_async_copy(base_hbm, base, lsem.at[0]),
        pltpu.make_async_copy(turn_hbm.at[gy], turn, lsem.at[1]),
    ]
    cells_in = pltpu.make_async_copy(h_hbm, hbuf, lsem.at[2])
    weights_in = pltpu.make_async_copy(w_hbm, wraw, lsem.at[3])
    loads = [
        pltpu.make_async_copy(skw_hbm, skw, lsem.at[4]),
        pltpu.make_async_copy(bias_hbm, par.at[0], lsem.at[5]),
        pltpu.make_async_copy(gain_hbm, par.at[1], lsem.at[6]),
        pltpu.make_async_copy(shift_hbm, par.at[2], lsem.at[7]),
        pltpu.make_async_copy(first_hbm.at[gx], first, lsem.at[8]),
    ]
    for cp in [*tables, cells_in, weights_in, *loads]:
        cp.start()

    def landed(ref, sem):
        pltpu.make_async_copy(ref, ref, sem).wait()

    barrier = pltpu.get_barrier_semaphore()
    for dy, dz in FAR_X:
        pl.semaphore_signal(barrier, 1, device_id={"gx": x_peer(dy, dz)}, device_id_type=MESH)
    for k in FAR_Y:
        pl.semaphore_signal(barrier, 1, device_id={"gy": (gy + k) % GY}, device_id_type=MESH)
    for k in FAR_COL:
        pl.semaphore_signal(
            barrier, 1, device_id={"col": (y_hi + k) % 4 * 2 + core}, device_id_type=MESH
        )
    pl.semaphore_signal(barrier, 1, device_id={"col": sibling}, device_id_type=MESH)

    for cp in tables:
        cp.wait()

    def table_row(y):
        for k in range(GY):
            cosine = turn[y * GY + k : y * GY + k + 1, :]
            sine = turn[(TY + y) * GY + k : (TY + y) * GY + k + 1, :]
            table[y, k] = (base[0] * cosine + base[1] * sine).astype(BF16)

    for y in range(EARLY_ROWS):
        table_row(y)
    cells_in.wait()
    for y in range(EARLY_ROWS, TY):
        table_row(y)
    cells = jnp.concatenate([hbuf[:, y].reshape(TX * C, N) for y in range(TY)], axis=1)
    steps = [table[:, k].reshape(TY * N, LANES) for k in range(GY)]
    local = jnp.dot(cells, jnp.concatenate(steps, axis=1), preferred_element_type=F32)
    for k in range(GY):
        part = local[:, k * LANES : (k + 1) * LANES].astype(BF16).reshape(TX, 2, HALF, LANES)
        for half in range(2):
            zsend[k, half] = part[:, half]

    pl.semaphore_wait(barrier, len(FAR_X) + len(FAR_Y) + len(FAR_COL) + 1)

    for half in range(2):
        for k in FAR_Y:
            pltpu.make_async_remote_copy(
                zsend.at[k, half], arecv.at[half, k - 1], asend.at[0], arcv.at[half],
                device_id={"gy": (gy + k) % GY}, device_id_type=MESH,
            ).start()

    weights_in.wait()
    for d in range(C // COL):
        block = jnp.concatenate(
            [wraw[k, s, d].astype(F32) for s in range(2) for k in range(KY)], axis=0
        )
        wbuf[col, d] = block.T.astype(BF16)
    for k in FAR_COL:
        pltpu.make_async_remote_copy(
            wbuf.at[col], wbuf.at[col], wsend.at[0], wrcv.at[0],
            device_id={"col": (y_hi + k) % 4 * 2 + core}, device_id_type=MESH,
        ).start()

    def to_sibling(slot):
        pltpu.make_async_remote_copy(
            wbuf.at[slot], wbuf.at[slot], vsend.at[0], vrcv.at[0],
            device_id={"col": sibling}, device_id_type=MESH,
        ).start()

    to_sibling(col)

    for cp in loads:
        cp.wait()
    wide = [jnp.broadcast_to(par[i], (N, C)).T for i in range(3)]
    affine_ref[0] = wide[1] * math.sqrt(0.5 * C)
    affine_ref[1] = wide[2] * math.sqrt(0.5)
    bias = wide[0] - jnp.mean(wide[0], axis=0, keepdims=True)
    pick = (
        lax.broadcasted_iota(jnp.int32, (C, TX * C), 1) % C
        == lax.broadcasted_iota(jnp.int32, (C, TX * C), 0)
    )
    spread = jnp.dot(skw[...], pick.astype(F32).astype(BF16), preferred_element_type=F32)
    spread = jnp.broadcast_to(spread[None], (TX, C, TX * C)).reshape(TX * C, TX * C)
    same = (
        lax.broadcasted_iota(jnp.int32, (TX * C, TX * C), 0) // C
        == lax.broadcasted_iota(jnp.int32, (TX * C, TX * C), 1) // C
    )
    diagonal = jnp.where(same, spread, 0.0).astype(BF16)

    def skip_rows(i, carry):
        four = [hbuf[:, 4 * i + j].reshape(TX * C, N) for j in range(4)]
        out = jnp.dot(diagonal, jnp.concatenate(four, axis=1), preferred_element_type=F32)
        for j in range(4):
            value = out[:, j * N : (j + 1) * N].reshape(TX, C, N)
            value = value - jnp.mean(value, axis=1, keepdims=True) + bias[None]
            skip_early[4 * i + j] = value[:XH]
            skip_late[4 * i + j] = value[XH:]
        return carry

    lax.fori_loop(0, TY // 4, skip_rows, 0)

    for half in range(2):
        landed(arecv.at[half], arcv.at[half])
        here, there = [], []
        for x in range(TX):
            v = zsend[0, half, x].astype(F32)
            for k in range(3):
                v = v + arecv[half, k, x].astype(F32)
            here.append(v)
            there.append(turned(v))
        for f in range(M // 2 + 1):
            even = odd = None
            for x in range(TX):
                if f == 0:
                    even = here[x] if even is None else even + here[x]
                    continue
                r = f * TX + x
                a = here[x] * first[r : r + 1, :]
                b = there[x] * first[9 * TX + r : 9 * TX + r + 1, :]
                even = a if even is None else even + a
                odd = b if odd is None else odd + b
            if f == 0:
                pm[half, 0] = even.astype(BF16)
                continue
            if f < M // 2:
                pm[half, f] = (even + odd).astype(BF16)
            pm[half, M - f] = (even - odd).astype(BF16)
        for i, (dy, dz) in enumerate(FAR_X):
            to = x_peer(dy, dz)
            pltpu.make_async_remote_copy(
                pm.at[half, to], brecv.at[half, i], bsend.at[0], brcv.at[half],
                device_id={"gx": to}, device_id_type=MESH,
            ).start()

    landed(wbuf.at[0:3], wrcv.at[0])
    for k in FAR_COL:
        to_sibling((y_hi + 4 - k) % 4 * 2 + core)

    scale = 1.0 / math.sqrt(N * N * N)
    for half in range(2):
        total = pm[half, gx].astype(F32)
        landed(brecv.at[half], brcv.at[half])
        for i in range(len(FAR_X)):
            total = total + brecv[half, i].astype(F32)
        spec[half * HALF : (half + 1) * HALF, :] = (total * scale).astype(BF16).astype(F32)
    landed(wbuf.at[0:4], vrcv.at[0])

    straight = spec[...]
    crossed = pltpu.roll(straight, LANES // 2, 1)
    lane = lax.broadcasted_iota(jnp.int32, (8, LANES), 1)
    for g in range(4):
        weight = wbuf[2 * g : 2 * g + 2].astype(F32).reshape(8, C, LANES)
        a = jnp.sum(weight * straight[None], axis=1)
        b = jnp.sum(weight * crossed[None], axis=1)
        mixed = jnp.where(
            lane < LANES // 2, a - pltpu.roll(a, LANES // 2, 1), b + pltpu.roll(b, LANES // 2, 1)
        )
        mixf[8 * g : 8 * g + 8, :] = mixed
    mixed = mixf[...]
    mixed = (mixed - jnp.mean(mixed, axis=0, keepdims=True)) * (1.0 / math.sqrt(M * M * M))
    mixed = mixed.astype(BF16)

    mrecv[gx] = mixed
    for dy, dz in FAR_X:
        pltpu.make_async_remote_copy(
            mrecv.at[gx], mrecv.at[gx], csend.at[0], crcv.at[0],
            device_id={"gx": x_peer(dy, dz)}, device_id_type=MESH,
        ).start()

    def table_column(y, carry):
        for k in range(GY):
            back_ref[y, k] = table[y, k].T
        return carry

    lax.fori_loop(0, TY, table_column, 0)

    landed(mrecv.at[0 : GX - 1], crcv.at[0])
    for late, rows in enumerate((rows_early, rows_late)):
        for half in range(2):
            part = slice(half * HALF, (half + 1) * HALF)
            zero = mrecv[0, part].astype(F32)
            out = [zero for _ in range(XH)]
            for f in range(1, M // 2 + 1):
                low = mrecv[M - f, part].astype(F32)
                if f < M // 2:
                    high = mrecv[f, part].astype(F32)
                    even, odd = high + low, turned(low - high)
                else:
                    even, odd = low, turned(low)
                for x in range(XH):
                    r = f * TX + late * XH + x
                    out[x] = out[x] + even * first[r : r + 1, :]
                    out[x] = out[x] + odd * first[9 * TX + r : 9 * TX + r + 1, :]
            for x in range(XH):
                rows[0, x, part, :] = out[x].astype(BF16)
        for k in FAR_Y:
            pltpu.make_async_remote_copy(
                rows.at[0], rows.at[k], dsend.at[0], drcv.at[late],
                device_id={"gy": (gy + GY - k) % GY}, device_id_type=MESH,
            ).start()

    landed(rows_early.at[1:4], drcv.at[0])
    settle(rows_early, back_ref, skip_early, affine_ref, out_early)

    landed(zsend.at[1:4], asend.at[0])
    landed(wbuf.at[0:3], wsend.at[0])
    landed(wbuf.at[0:4], vsend.at[0])
    landed(brecv, bsend.at[0])
    landed(mrecv.at[0 : GX - 1], csend.at[0])
    landed(zsend.at[1:4], dsend.at[0])
    landed(rows_late.at[1:4], drcv.at[1])


def settle(rows_ref, back_ref, skip_ref, affine_ref, out_ref, written=None):
    rows = jnp.concatenate([rows_ref[k].reshape(XH * C, LANES) for k in range(GY)], axis=1)
    for y in range(0, TY, 2):
        back = [back_ref[y + j].reshape(PEER, N) for j in range(2)]
        both = jnp.dot(rows, jnp.concatenate(back, axis=1), preferred_element_type=F32)
        for j in range(2):
            for x in range(XH):
                value = both[x * C : (x + 1) * C, j * N : (j + 1) * N] + skip_ref[y + j, x]
                spread = jnp.sum(value * value, axis=0, keepdims=True)
                value = value * lax.rsqrt(spread + C * NORM_EPS) * affine_ref[0] + affine_ref[1]
                value = (value * math.sqrt(0.5)) * (lax.erf(value) + 1.0)
                out_ref[x, y + j] = value.astype(BF16)
        if written is not None and y % WRITE == WRITE - 2:
            written(pl.ds(y + 2 - WRITE, WRITE))


def finish_kernel(
    rows_late, back_ref, skip_late, affine_ref, out_early, out_hbm, out_late, early_sem, late_sem
):
    early = pltpu.make_async_copy(out_early, out_hbm.at[0:XH], early_sem.at[0])
    early.start()

    def written(span):
        pltpu.make_async_copy(
            out_late.at[:, span], out_hbm.at[XH:TX, span], late_sem.at[0]
        ).start()

    settle(rows_late, back_ref, skip_late, affine_ref, out_late, written)
    early.wait()
    pltpu.make_async_copy(out_late, out_hbm.at[XH:TX], late_sem.at[0]).wait()


def local(fields, spectral, skip_weight, skip_bias, norm_gain, norm_shift):
    weights = jnp.transpose(spectral[0, 0], (0, 1, 3, 4, 2))
    dma = pltpu.SemaphoreType.DMA
    anywhere = pl.BlockSpec(memory_space=pltpu.HBM)
    vmem = pl.BlockSpec(memory_space=pltpu.VMEM)
    far_x = len(FAR_X)
    rows, back, skip, affine, early = pl.pallas_call(
        modes_kernel,
        name="modes",
        out_shape=[
            pltpu.VMEM((GY, XH, C, LANES), BF16),
            pltpu.VMEM((TY, GY, LANES, N), BF16),
            pltpu.VMEM((TY, XH, C, N), F32),
            pltpu.VMEM((2, C, N), F32),
            pltpu.VMEM((XH, TY, C, N), BF16),
        ],
        in_specs=[anywhere] * 9,
        out_specs=[vmem] * 5,
        scratch_shapes=[
            pltpu.VMEM((GY, XH, C, LANES), BF16),
            pltpu.VMEM((TY, XH, C, N), F32),
            pltpu.VMEM((TY, GY, N, LANES), BF16),
            pltpu.VMEM((TX, TY, C, N), BF16),
            pltpu.VMEM((KY, 2, C // COL, M, C), BF16),
            pltpu.VMEM((C, C), BF16),
            pltpu.VMEM((3, 1, C), F32),
            pltpu.VMEM((2, N, LANES), F32),
            pltpu.VMEM((2 * TY * GY, LANES), F32),
            pltpu.VMEM((2 * 9 * TX, LANES), F32),
            pltpu.VMEM((GY, 2, TX, HALF, LANES), BF16),
            pltpu.VMEM((2, 3, TX, HALF, LANES), BF16),
            pltpu.VMEM((2, M, HALF, LANES), BF16),
            pltpu.VMEM((2, far_x, HALF, LANES), BF16),
            pltpu.VMEM((C, LANES), F32),
            pltpu.VMEM((C, LANES), F32),
            pltpu.VMEM((COL, C // COL, C, LANES), BF16),
            pltpu.VMEM((GX, C, LANES), BF16),
            dma((9,)),
            dma((1,)), dma((2,)),
            dma((1,)), dma((2,)),
            dma((1,)), dma((1,)),
            dma((1,)), dma((2,)),
            dma((1,)), dma((1,)),
            dma((1,)), dma((1,)),
        ],
        compiler_params=pltpu.CompilerParams(
            collective_id=0, has_side_effects=True, vmem_limit_bytes=48 << 20
        ),
    )(
        fields[0], weights, skip_weight[0], skip_bias, norm_gain, norm_shift,
        jnp.asarray(base_tables()), jnp.asarray(turn_tables()), jnp.asarray(first_tables()),
    )
    out = pl.pallas_call(
        finish_kernel,
        name="finish",
        out_shape=jax.ShapeDtypeStruct((TX, TY, C, N), BF16),
        in_specs=[vmem] * 5,
        out_specs=anywhere,
        scratch_shapes=[pltpu.VMEM((XH, TY, C, N), BF16), dma((1,)), dma((1,))],
        compiler_params=pltpu.CompilerParams(vmem_limit_bytes=16 << 20),
    )(rows, back, skip, affine, early)
    return out[None]


def solution(mesh):
    placed = (
        P("col", "gx", "gy", None, None),
        P(None, "gx", "gy", None, None, "col", None),
        P(),
        P(),
        P(),
        P(),
    )
    return jax.shard_map(
        local,
        mesh=mesh,
        in_specs=placed,
        out_specs=P("col", "gx", "gy", None, None),
        check_vma=False,
    )
```
